256 devices in a mesh: gx: 32 (over y, z), gy: 8 (over x, core).
Axes of the slice: x: 4, y: 4, z: 8, core: 2. Of those that a mesh axis runs over, the one named last changes fastest.
Arguments:
- loads: float32 [64, 393216], P(None, ('gx', 'gy')), may hold values from -6 to 6
- guess: float32 [64, 393216], P(None, ('gx', 'gy')), may hold values from -4 to 4
- mass: float32 [393216], P(('gx', 'gy')), may hold values from 0.5 to 4
- moduli: float32 [393216], P(('gx', 'gy')), may hold values from 0.3 to 3
- tiles: float32 [10240, 256, 256], P(('gx', 'gy')), may hold values from -0.21875 to 0.21875
- tile_row: int32 [10240], P(('gx', 'gy')), may hold values from -1 to 5, as said below
- tile_col: int32 [10240], P(('gx', 'gy')), may hold values from 0 to 21, as said below
- send_list: int32 [256, 4, 4], P(('gx', 'gy')), may hold values from -1 to 5, as said below
Outputs:
- solution: float32 [64, 393216], P(None, ('gx', 'gy'))
- residual: float32 [64, 393216], P(None, ('gx', 'gy'))
The draws below stay inside these ranges and needn't reach their ends.
Inputs may be any that keep to these rules, and one draw needn't show every extreme that they name: `tile_row`: strain block (of the tile's own device) of each slot, -1 for an unused slot. A device's used slots come first; slot r below 6 holds the diagonal tile of block r; some device uses all 40 slots. `tile_col`: column block of each slot in its device's extended numbering: below 6 an own block; 6 + g * 4 + k the k-th entry of the list that neighbour g (0 below along gx, 1 above along gx, 2 below along gy, 3 above along gy) sends to this device. Used slots read only entries that are not -1, every such entry is read by some slot, unused slots hold 0. `send_list`: for each device and each neighbour in the order below gx, above gx, below gy, above gy: distinct own blocks to send, padded with -1 at the end; all -1 toward a missing neighbour; some lists are full.
All inputs are finite; a program needn't handle non-finite values.
Results may differ from the reference program's by a relative error of at most 0.0003.
Values sent between devices are 32-bit elements; how exact they have to be, the bound alone decides.
A program may use at most 128 MiB of HBM per device.

```python
import math
import jax
import jax.numpy as jnp
from jax import lax

TB = 256
RB = 6
HALO = 4
TILE_SLOTS = 40
NRHS = 64
ITERS = 2
DOFS = 393216
TILES = 10240
N_GX = 32
N_GY = 8


def layout(key):
    devices_all = N_GX * N_GY
    flat = jnp.arange(devices_all, dtype=jnp.int32)
    along_x = flat // N_GY
    along_y = flat % N_GY
    counts = jax.random.randint(jax.random.fold_in(key, 101), (devices_all, 4), 1, HALO + 1)
    counts = jnp.where((flat % 5 == 0)[:, None], HALO, counts)
    present = jnp.stack([along_x > 0, along_x < N_GX - 1, along_y > 0, along_y < N_GY - 1], axis=1)
    counts = jnp.where(present, counts, 0).astype(jnp.int32)
    scores = jax.random.randint(jax.random.fold_in(key, 102), (devices_all, 4, RB), 0, 1 << 20) * RB + jnp.arange(RB, dtype=jnp.int32)
    order = jnp.argsort(scores, axis=-1)[:, :, :HALO].astype(jnp.int32)
    send_list = jnp.where(jnp.arange(HALO, dtype=jnp.int32) < counts[:, :, None], order, -1)
    grid = counts.reshape(N_GX, N_GY, 4)
    zero_row = jnp.zeros((1, N_GY), jnp.int32)
    zero_col = jnp.zeros((N_GX, 1), jnp.int32)
    from_lower_x = jnp.concatenate([zero_row, grid[:-1, :, 1]], 0)
    from_upper_x = jnp.concatenate([grid[1:, :, 0], zero_row], 0)
    from_lower_y = jnp.concatenate([zero_col, grid[:, :-1, 3]], 1)
    from_upper_y = jnp.concatenate([grid[:, 1:, 2], zero_col], 1)
    incoming = jnp.stack([from_lower_x, from_upper_x, from_lower_y, from_upper_y], -1).reshape(devices_all, 4)
    halo_index = jnp.arange(4 * HALO, dtype=jnp.int32)
    halo_live = (halo_index % HALO)[None, :] < incoming[:, halo_index // HALO]
    column_live = jnp.concatenate([jnp.ones((devices_all, RB), bool), halo_live], 1)
    needed = RB + jnp.sum(incoming, axis=1)
    spare = TILE_SLOTS - needed + 1
    extra_one = jax.random.randint(jax.random.fold_in(key, 103), (devices_all,), 0, spare)
    extra_two = jax.random.randint(jax.random.fold_in(key, 104), (devices_all,), 0, spare)
    extra_three = jax.random.randint(jax.random.fold_in(key, 105), (devices_all,), 0, spare)
    extra = jnp.minimum(jnp.minimum(extra_one, extra_two), extra_three)
    live = jnp.where(flat % 5 == 0, TILE_SLOTS, needed + extra)
    slot = jnp.arange(TILE_SLOTS, dtype=jnp.int32)
    halo_rank = jnp.clip(slot - RB, 0, None)[None, :]
    halo_cum = jnp.cumsum(halo_live.astype(jnp.int32), axis=1)
    halo_column = RB + jnp.sum((halo_cum[:, None, :] <= halo_rank[:, :, None]).astype(jnp.int32), axis=-1)
    count_live = jnp.sum(column_live.astype(jnp.int32), axis=1)
    pick = jax.random.randint(jax.random.fold_in(key, 107), (devices_all, TILE_SLOTS), 0, count_live[:, None])
    live_cum = jnp.cumsum(column_live.astype(jnp.int32), axis=1)
    random_column = jnp.sum((live_cum[:, None, :] <= pick[:, :, None]).astype(jnp.int32), axis=-1)
    random_row = jax.random.randint(jax.random.fold_in(key, 108), (devices_all, TILE_SLOTS), 0, RB)
    rows = jnp.where(slot < RB, slot, jnp.where(slot < live[:, None], random_row, -1))
    columns = jnp.where(slot < RB, slot, jnp.where(slot < needed[:, None], halo_column, jnp.where(slot < live[:, None], random_column, 0)))
    return (rows.reshape(-1).astype(jnp.int32), columns.reshape(-1).astype(jnp.int32), send_list.astype(jnp.int32))


def draw_tile_row(key, part):
    return layout(key)[0]


def draw_tile_col(key, part):
    return layout(key)[1]


def draw_send_list(key, part):
    return layout(key)[2]


def shard_levels(stream_key, shape, shards, smallest, largest):
    factor_of = 1.0
    for dim, shards_of in shards:
        draws = jax.random.uniform(jax.random.fold_in(jax.random.fold_in(stream_key, 6), dim), (shards_of,), jnp.float32, smallest / len(shards), largest / len(shards))
        factor_of = factor_of * jnp.repeat(jnp.exp(draws), shape[dim] // shards_of).reshape((-1,) + (1,) * (len(shape) - 1 - dim))
    return factor_of


def scatter_about(stream_key, shape, scale, bound, pieces=(), kind=jnp.bfloat16):
    drawn = scale * jax.random.normal(stream_key, shape, jnp.float32)
    if pieces:
        drawn = drawn * shard_levels(stream_key, shape, pieces, -0.22, 0.18)
    return jnp.clip(drawn, -bound, bound).astype(kind)


def setup_inputs(seed: int = 0) -> dict:
    key_of = jax.random.split(jax.random.key(seed), 9)
    return {
        "loads": scatter_about(key_of[0], (NRHS, DOFS), 1.0, 6.0, ((1, 256),), jnp.float32),
        "guess": scatter_about(key_of[1], (NRHS, DOFS), 0.5, 4.0, ((1, 256),), jnp.float32),
        "mass": jnp.clip(jnp.exp(math.log(4.0) - 2.0794415 * jax.random.uniform(key_of[2], (DOFS,), jnp.float32) ** shard_levels(key_of[2], (DOFS,), ((0, 256),), -0.2, 0.2)), 0.5, 4.0),
        "moduli": jnp.clip(jnp.exp(math.log(3.0) - 2.3025851 * jax.random.uniform(key_of[3], (DOFS,), jnp.float32) ** shard_levels(key_of[3], (DOFS,), ((0, 256),), -0.2, 0.2)), 0.3, 3.0),
        "tiles": scatter_about(key_of[4], (TILES, TB, TB), (TB * 3) ** -0.5, 0.21875, ((0, 256),), jnp.float32),
        "tile_row": draw_tile_row(jax.random.fold_in(key_of[8], 71), 0),
        "tile_col": draw_tile_col(jax.random.fold_in(key_of[8], 71), 0),
        "send_list": draw_send_list(jax.random.fold_in(key_of[8], 71), 0),
    }


def local_terms(operands):
    own, incoming, tiles_dev, rows_dev, cols_dev, moduli_dev = operands
    precise = lax.Precision.HIGHEST
    extent = RB + 4 * HALO
    extended = jnp.concatenate([own, jnp.transpose(incoming, (1, 0, 2))], 1)
    picked = jnp.take(extended, cols_dev, axis=1)
    row_onehot = (rows_dev[:, None] == jnp.arange(RB, dtype=jnp.int32)[None, :]).astype(jnp.float32)
    col_onehot = (cols_dev[:, None] == jnp.arange(extent, dtype=jnp.int32)[None, :]).astype(jnp.float32)
    strain_tiles = jnp.einsum("tij,ktj->kti", tiles_dev, picked, precision=precise)
    strain = jnp.einsum("tr,kti->kri", row_onehot, strain_tiles, precision=precise)
    stress = moduli_dev[None] * strain
    spread = jnp.einsum("tr,kri->kti", row_onehot, stress, precision=precise)
    pulled = jnp.einsum("tij,kti->ktj", tiles_dev, spread, precision=precise)
    return jnp.einsum("te,ktj->ekj", col_onehot, pulled, precision=precise)


def reference(loads, guess, mass, moduli, tiles, tile_row, tile_col, send_list):
    precise = lax.Precision.HIGHEST
    devices_all = N_GX * N_GY
    tiles_dev = tiles.reshape(devices_all, TILE_SLOTS, TB, TB)
    rows_dev = tile_row.reshape(devices_all, TILE_SLOTS)
    cols_dev = tile_col.reshape(devices_all, TILE_SLOTS)
    moduli_dev = moduli.reshape(devices_all, RB, TB)
    mass_dev = mass.reshape(devices_all, RB, TB)
    list_onehot = (send_list[:, :, :, None] == jnp.arange(RB, dtype=jnp.int32)).astype(jnp.float32)

    def shifted(grid, lower_src, upper_src, axis):
        if axis == 0:
            lower = jnp.concatenate([jnp.zeros_like(grid[:1, :, lower_src]), grid[:-1, :, lower_src]], 0)
            upper = jnp.concatenate([grid[1:, :, upper_src], jnp.zeros_like(grid[:1, :, upper_src])], 0)
        else:
            lower = jnp.concatenate([jnp.zeros_like(grid[:, :1, lower_src]), grid[:, :-1, lower_src]], 1)
            upper = jnp.concatenate([grid[:, 1:, upper_src], jnp.zeros_like(grid[:, :1, upper_src])], 1)
        return lower, upper

    def operate(vector):
        own = jnp.transpose(vector.reshape(NRHS, devices_all, RB, TB), (1, 0, 2, 3))
        packs = jnp.einsum("fdhr,fkri->fdhki", list_onehot, own, precision=precise)
        grid = packs.reshape(N_GX, N_GY, 4, HALO, NRHS, TB)
        first, second = shifted(grid, 1, 0, 0)
        third, fourth = shifted(grid, 3, 2, 1)
        incoming = jnp.stack([first, second, third, fourth], 2).reshape(devices_all, 4 * HALO, NRHS, TB)
        gathered = lax.map(local_terms, (own, incoming, tiles_dev, rows_dev, cols_dev, moduli_dev))
        returns = gathered[:, RB:].reshape(N_GX, N_GY, 4, HALO, NRHS, TB)
        first, second = shifted(returns, 1, 0, 0)
        third, fourth = shifted(returns, 3, 2, 1)
        returned = jnp.stack([first, second, third, fourth], 2).reshape(devices_all, 4, HALO, NRHS, TB)
        total = gathered[:, :RB] + jnp.einsum("fdhr,fdhki->frki", list_onehot, returned, precision=precise)
        result = mass_dev[:, None] * own + jnp.transpose(total, (0, 2, 1, 3))
        return jnp.transpose(result, (1, 0, 2, 3)).reshape(NRHS, devices_all * RB * TB)

    solution = guess
    residual = loads - operate(guess)
    direction = residual
    norm_now = jnp.sum(residual * residual, axis=1)
    for step in range(ITERS):
        image = operate(direction)
        alpha = norm_now / jnp.sum(direction * image, axis=1)
        solution = solution + alpha[:, None] * direction
        residual = residual - alpha[:, None] * image
        if step + 1 < ITERS:
            norm_next = jnp.sum(residual * residual, axis=1)
            direction = residual + (norm_next / norm_now)[:, None] * direction
            norm_now = norm_next
    return solution, residual
```

```python
import functools

import jax
import jax.numpy as jnp
from jax import lax
from jax.experimental import pallas as pl
from jax.experimental.pallas import tpu as pltpu
from jax.sharding import PartitionSpec as P

MESH = pl.DeviceIdType.MESH
GROUPS = 2
CHUNKS = 8
UNROLL = 20
F32 = jnp.float32
BF16 = jnp.bfloat16


class Tables:
    def __init__(self, slots, blocks, depth):
        self.slots, self.blocks, self.depth = slots, blocks, depth
        self.extent = blocks + 4 * depth
        at = 0

        def take(n):
            nonlocal at
            start = at
            at += n
            return start

        self.row_slot = take(slots)
        self.row_col = take(slots)
        self.row_keep = take(slots + 8)
        self.col_slot = take(slots)
        self.col_row = take(slots)
        self.col_keep = take(slots + 8)
        self.row_last = take(blocks + 2)
        self.col_last = take(self.extent + 2)
        self.col_has = take(self.extent + 2)
        self.pack_at = take(4 * depth)
        self.pack_has = take(4 * depth)
        self.back_at = take(4 * blocks + 8)
        self.back_has = take(4 * blocks + 8)
        self.size = -(-at // 128) * 128


def index_kernel(tb, row_ref, col_ref, list_ref, out_ref, first_ref, next_ref):
    slots, blocks, depth, extent = tb.slots, tb.blocks, tb.depth, tb.extent

    def row_key(t):
        row = row_ref[t]
        return jnp.where(row < 0, blocks, row)

    def col_key(t):
        return jnp.where(row_ref[t] < 0, extent, col_ref[t])

    def sort(key, keys, slot_at, other_at, keep_at, other):
        for k in range(keys + 1):
            next_ref[k] = 0

        def count(t, c):
            k = key(t)
            next_ref[k] = next_ref[k] + 1
            return c

        lax.fori_loop(0, slots, count, 0, unroll=True)
        at = jnp.int32(0)
        for k in range(keys + 1):
            n = next_ref[k]
            first_ref[k] = at
            next_ref[k] = at
            at = at + n

        def place(t, c):
            k = key(t)
            p = next_ref[k]
            next_ref[k] = p + 1
            out_ref[slot_at + p] = t
            out_ref[other_at + p] = other(t)
            out_ref[keep_at + p] = 1
            return c

        lax.fori_loop(0, slots, place, 0, unroll=True)
        for k in range(keys + 1):
            out_ref[keep_at + first_ref[k]] = 0

    sort(row_key, blocks, tb.row_slot, tb.row_col, tb.row_keep, lambda t: col_ref[t])
    for k in range(blocks):
        out_ref[tb.row_last + k] = jnp.maximum(next_ref[k] - 1, 0)
    sort(col_key, extent, tb.col_slot, tb.col_row, tb.col_keep, lambda t: jnp.maximum(row_ref[t], 0))
    for k in range(extent):
        out_ref[tb.col_last + k] = jnp.maximum(next_ref[k] - 1, 0)
        out_ref[tb.col_has + k] = jnp.where(next_ref[k] > first_ref[k], 1, 0)
    for k in range(4 * blocks + 8):
        out_ref[tb.back_at + k] = 0
        out_ref[tb.back_has + k] = 0
    for d in range(4):
        for h in range(depth):
            r = list_ref[0, d, h]
            has = jnp.where(r >= 0, 1, 0)
            out_ref[tb.pack_at + d * depth + h] = jnp.maximum(r, 0)
            out_ref[tb.pack_has + d * depth + h] = has
            spot = jnp.where(r >= 0, d * blocks + r, 4 * blocks)
            out_ref[tb.back_at + spot] = h
            out_ref[tb.back_has + spot] = has


def halves(value):
    high = value.astype(BF16)
    return high, (value - high.astype(F32)).astype(BF16)


def solve_kernel(
    tb, n_gx, n_gy, n_z,
    tab, mass, moduli, guess, loads, tiles,
    sol, res,
    stage, tile, tile_t, hist, ext, stress, scan, own, strain0, norm0, coef,
    send_f, recv_f, send_r, recv_r, red_send, red_recv,
    tile_sem, fs_sem, fr_sem, rs_sem, rr_sem, ds_sem, dr_sem,
):
    slots, blocks, depth = tb.slots, tb.blocks, tb.depth
    block = mass.shape[1] // blocks
    rows = hist.shape[3]
    groups = range(GROUPS)
    gx, gy = lax.axis_index("gx"), lax.axis_index("gy")
    n_y = n_gx // n_z
    y, z = gx // n_z, gx % n_z

    def chip(yy, zz):
        return yy * n_z + zz

    around = [
        ((gx + n_gx - 1) % n_gx, gy),
        ((gx + 1) % n_gx, gy),
        (gx, (gy + n_gy - 1) % n_gy),
        (gx, (gy + 1) % n_gy),
    ]
    phases = [
        [(gx, (gy + k) % n_gy) for k in range(1, n_gy)],
        [(chip((y + k) % n_y, z), gy) for k in range(1, n_y)],
        [(chip(y, (z + k) % n_z), gy) for k in range(1, n_z)],
    ]
    starts = [0, len(phases[0]), len(phases[0]) + len(phases[1])]

    per = slots // CHUNKS
    loads_in = [
        pltpu.make_async_copy(tiles.at[pl.ds(c * per, per)], stage.at[pl.ds(c * per, per)], tile_sem.at[c])
        for c in range(CHUNKS)
    ]
    for copy in loads_in:
        copy.start()

    barrier = pltpu.get_barrier_semaphore()
    greet = around[:2] + phases[0] + phases[1] + phases[2]
    for device in greet:
        pl.semaphore_signal(barrier, inc=1, device_id=device, device_id_type=MESH)

    def flag(at):
        return tab[at].astype(F32)

    def lanes(ref, b):
        return ref[:, b * block : (b + 1) * block]

    def forward(g, d):
        return pltpu.make_async_remote_copy(
            src_ref=send_f.at[g, d],
            dst_ref=recv_f.at[g, d ^ 1],
            send_sem=fs_sem.at[g, d],
            recv_sem=fr_sem.at[g, d ^ 1],
            device_id=around[d],
            device_id_type=MESH,
        )

    def backward(g, d):
        return pltpu.make_async_remote_copy(
            src_ref=send_r.at[g, d],
            dst_ref=recv_r[g].at[d ^ 1],
            send_sem=rs_sem.at[g, d],
            recv_sem=rr_sem.at[g, d ^ 1],
            device_id=around[d],
            device_id_type=MESH,
        )

    def wait_recv(make, g):
        for d in range(4):
            make(g, d ^ 1).wait_recv()

    def pack(step, g):
        for d in range(4):
            for h in range(depth):
                k = d * depth + h
                send_f[g, d, h] = hist[step, g, tab[tb.pack_at + k]] * flag(tb.pack_has + k)

    def split_own(step, g):
        for b in range(blocks):
            high, low = halves(hist[step, g, b])
            ext[g, b, :rows] = high
            ext[g, b, rows:] = low

    def split_halo(g):
        for d in range(4):
            for h in range(depth):
                high, low = halves(recv_f[g, d, h])
                ext[g, blocks + d * depth + h, :rows] = high
                ext[g, blocks + d * depth + h, rows:] = low

    def sweep(source, g, weights, slot_at, block_at, keep_at):
        def body(i, total):
            for u in range(UNROLL):
                t = i * UNROLL + u
                x = source[g, tab[block_at + t]]
                both = jnp.dot(
                    jnp.concatenate([x, x], axis=1), weights[tab[slot_at + t]], preferred_element_type=F32
                )
                total = total * flag(keep_at + t) + (both[:rows] + both[rows:])
                scan[t] = total
            return total

        lax.fori_loop(0, slots // UNROLL, body, jnp.zeros((rows, block), F32))

    def strain_pass(step, g):
        sweep(ext, g, tile_t, tb.row_slot, tb.row_col, tb.row_keep)
        square = jnp.zeros((rows, block), F32)
        energy = jnp.zeros((rows, block), F32)
        if step == 2:
            alpha = jnp.concatenate([coef[g, 0], coef[g, 0]], axis=1)
        for b in range(blocks):
            strain = scan[tab[tb.row_last + b]]
            module = lanes(moduli, b)
            value = module * strain
            high, low = halves(value)
            stress[g, b, :rows] = high
            stress[g, b, rows:] = low
            if step == 1:
                strain0[g, b] = strain
                r = hist[1, g, b]
                square += r * r
                energy += value * strain + lanes(mass, b) * (r * r)
            if step == 2:
                r = hist[1, g, b] - alpha * hist[2, g, b]
                mixed = strain0[g, b] - alpha * strain
                square += r * r
                energy += module * (mixed * mixed) + lanes(mass, b) * (r * r)
        return square, energy

    def back_pass(step, g):
        sweep(stress, g, tile, tb.col_slot, tb.col_row, tb.col_keep)
        if step > 0:
            for d in range(4):
                backward(g, d).wait_send()
        for d in range(4):
            for h in range(depth):
                e = blocks + d * depth + h
                send_r[g, d, h] = scan[tab[tb.col_last + e]] * flag(tb.col_has + e)
        for d in range(4):
            backward(g, d).start()
        for b in range(blocks):
            own[g, b] = scan[tab[tb.col_last + b]] * flag(tb.col_has + b) + lanes(mass, b) * hist[step, g, b]

    def total_of(g, b):
        total = own[g, b]
        for d in range(4):
            k = d * blocks + b
            total += recv_r[g][d, tab[tb.back_at + k]] * flag(tb.back_has + k)
        return total

    def reduce_copies(which, g, phase):
        return [
            pltpu.make_async_remote_copy(
                src_ref=red_send.at[which, g, phase],
                dst_ref=red_recv.at[which, g, starts[phase] + i],
                send_sem=ds_sem.at[which, g, starts[phase] + i],
                recv_sem=dr_sem.at[which, g, starts[phase] + i],
                device_id=device,
                device_id_type=MESH,
            )
            for i, device in enumerate(phases[phase])
        ]

    def reduce_start(which, g, square, energy):
        half = block // 2
        stacked = jnp.concatenate(
            [
                square[:, :half] + square[:, half:],
                energy[:, :half] + energy[:, half:],
                jnp.zeros((128 - 2 * rows, half), F32),
            ],
            axis=0,
        )
        red_send[which, g, 0] = jnp.sum(stacked.T, axis=0, keepdims=True)
        for copy in reduce_copies(which, g, 0):
            copy.start()

    def reduced(which, g, phase):
        value = red_send[which, g, phase]
        for i, copy in enumerate(reduce_copies(which, g, phase)):
            copy.wait_recv()
            value += red_recv[which, g, starts[phase] + i]
        return value

    def reduce_next(which, g, phase):
        red_send[which, g, phase + 1] = reduced(which, g, phase)
        for copy in reduce_copies(which, g, phase + 1):
            copy.start()

    def reduce_end(which, g):
        spread = jnp.broadcast_to(reduced(which, g, 2), (128, 128)).T
        return spread[:rows], spread[rows : 2 * rows]

    def wide(value):
        return jnp.concatenate([value, value], axis=1)

    for g in groups:
        for b in range(blocks):
            hist[0, g, b] = guess[g * rows : (g + 1) * rows, b * block : (b + 1) * block]
        pack(0, g)
    pl.semaphore_wait(barrier, len(greet))
    for g in groups:
        for d in range(4):
            forward(g, d).start()
        split_own(0, g)

    for c in range(CHUNKS):
        loads_in[c].wait()

        def split_tile(i, carry):
            t = c * per + i
            value = stage[t]
            high, low = halves(value)
            tile[t, :block] = high
            tile[t, block:] = low
            high, low = halves(value.T)
            tile_t[t, :block] = high
            tile_t[t, block:] = low
            return carry

        lax.fori_loop(0, per, split_tile, 0)

    def finish(step, g):
        wait_recv(backward, g)
        for b in range(blocks):
            value = total_of(g, b)
            if step == 0:
                value = loads[g * rows : (g + 1) * rows, b * block : (b + 1) * block] - value
            hist[step + 1, g, b] = value
        for d in range(4):
            forward(g, d).wait_send()
        pack(step + 1, g)
        for d in range(4):
            forward(g, d).start()
        split_own(step + 1, g)

    for step in range(2):
        for g in groups:
            wait_recv(forward, g)
            split_halo(g)
            square, energy = strain_pass(step, g)
            if step == 1:
                reduce_start(0, g, square, energy)
            back_pass(step, g)
        for g in groups:
            finish(step, g)
            if step == 1 and g == 0:
                for k in groups:
                    reduce_next(0, k, 0)
    for g in groups:
        reduce_next(0, g, 1)

    for g in groups:
        wait_recv(forward, g)
        split_halo(g)
        norm, curve = reduce_end(0, g)
        norm0[g] = norm
        coef[g, 0] = norm / curve
        square, energy = strain_pass(2, g)
        reduce_start(1, g, square, energy)
        back_pass(2, g)
    for g in groups:
        reduce_next(1, g, 0)
    for g in groups:
        reduce_next(1, g, 1)
    for g in groups:
        wait_recv(backward, g)
        norm, curve = reduce_end(1, g)
        alpha0 = coef[g, 0]
        beta = norm / norm0[g]
        alpha1 = norm / (curve - beta * norm / alpha0)
        alpha0, alpha1, beta = wide(alpha0), wide(alpha1), wide(beta)
        for b in range(blocks):
            r0, w1 = hist[1, g, b], hist[2, g, b]
            w2 = total_of(g, b)
            r1 = r0 - alpha0 * w1
            part = (slice(g * rows, (g + 1) * rows), slice(b * block, (b + 1) * block))
            sol[part] = hist[0, g, b] + alpha0 * r0 + alpha1 * (r1 + beta * r0)
            res[part] = r1 - alpha1 * (w1 - alpha0 * w2 + beta * w1)
    for g in groups:
        for d in range(4):
            forward(g, d).wait_send()
            backward(g, d).wait_send()
        for which in range(2):
            for phase in range(3):
                for copy in reduce_copies(which, g, phase):
                    copy.wait_send()


def solution(mesh):
    n_gx, n_gy = mesh.shape["gx"], mesh.shape["gy"]
    n_z = 8 if n_gx % 8 == 0 and n_gx > 8 else 2

    def on_device(loads, guess, mass, moduli, tiles, tile_row, tile_col, send_list):
        cases, width = loads.shape
        slots, block = tiles.shape[0], tiles.shape[1]
        depth = send_list.shape[2]
        blocks = width // block
        rows = cases // GROUPS
        tb = Tables(slots, blocks, depth)
        smem = pl.BlockSpec(memory_space=pltpu.SMEM)
        vmem = pl.BlockSpec(memory_space=pltpu.VMEM)
        table = pl.pallas_call(
            functools.partial(index_kernel, tb),
            out_shape=jax.ShapeDtypeStruct((tb.size,), jnp.int32),
            in_specs=[smem] * 3,
            out_specs=smem,
            scratch_shapes=[pltpu.SMEM((32,), jnp.int32), pltpu.SMEM((32,), jnp.int32)],
            name="index_tables",
        )(tile_row, tile_col, send_list)
        peers = (n_gy - 1) + (n_gx // n_z - 1) + (n_z - 1)
        halo = (GROUPS, 4, depth, rows, block)
        dma = pltpu.SemaphoreType.DMA
        return pl.pallas_call(
            functools.partial(solve_kernel, tb, n_gx, n_gy, n_z),
            out_shape=[jax.ShapeDtypeStruct((cases, width), F32)] * 2,
            in_specs=[smem, vmem, vmem, vmem, vmem, pl.BlockSpec(memory_space=pl.ANY)],
            out_specs=[vmem, vmem],
            scratch_shapes=[
                pltpu.VMEM((slots, block, block), F32),
                pltpu.VMEM((slots, 2 * block, block), BF16),
                pltpu.VMEM((slots, 2 * block, block), BF16),
                pltpu.VMEM((3, GROUPS, blocks, rows, block), F32),
                pltpu.VMEM((GROUPS, tb.extent, 2 * rows, block), BF16),
                pltpu.VMEM((GROUPS, blocks, 2 * rows, block), BF16),
                pltpu.VMEM((slots, rows, block), F32),
                pltpu.VMEM((GROUPS, blocks, rows, block), F32),
                pltpu.VMEM((GROUPS, blocks, rows, block), F32),
                pltpu.VMEM((GROUPS, rows, 128), F32),
                pltpu.VMEM((GROUPS, 1, rows, 128), F32),
                pltpu.VMEM(halo, F32),
                pltpu.VMEM(halo, F32),
                pltpu.VMEM(halo, F32),
                [pltpu.VMEM(halo[1:], F32)] * GROUPS,
                pltpu.VMEM((2, GROUPS, 3, 1, 128), F32),
                pltpu.VMEM((2, GROUPS, peers, 1, 128), F32),
                dma((CHUNKS,)),
                dma((GROUPS, 4)),
                dma((GROUPS, 4)),
                dma((GROUPS, 4)),
                dma((GROUPS, 4)),
                dma((2, GROUPS, peers)),
                dma((2, GROUPS, peers)),
            ],
            compiler_params=pltpu.CompilerParams(
                collective_id=0, has_side_effects=True, vmem_limit_bytes=60 * 1024 * 1024
            ),
            name="solve",
        )(table, mass.reshape(1, width), moduli.reshape(1, width), guess, loads, tiles)

    both = ("gx", "gy")
    return jax.shard_map(
        on_device,
        mesh=mesh,
        in_specs=(
            P(None, both), P(None, both), P(both), P(both), P(both, None, None), P(both), P(both), P(both, None, None),
        ),
        out_specs=(P(None, both), P(None, both)),
        check_vma=False,
    )
```

```python
import functools

import jax
import jax.numpy as jnp
from jax import lax
from jax.experimental import pallas as pl
from jax.experimental.pallas import tpu as pltpu
from jax.sharding import PartitionSpec as P

MESH = pl.DeviceIdType.MESH
GROUPS = 2
CHUNKS = 8
UNROLL = 20
F32 = jnp.float32
BF16 = jnp.bfloat16


ROW_SLOT, ROW_COL, ROW_KEEP, COL_SLOT, COL_ROW, COL_KEEP, ROW_LAST, COL_LAST, COL_HAS = range(9)


def sorted_slots(key_of, other, lane):
    code = (key_of * 64 + other) * 64 + lane
    across = jnp.broadcast_to(code, (128, 128))
    down = across.T
    place = jnp.sum((down < across).astype(jnp.int32), axis=0, keepdims=True)
    place = jnp.broadcast_to(place, (128, 128)).T
    spot = jnp.broadcast_to(lane, (128, 128))
    here = jnp.sum(jnp.where(place == spot, down, 0), axis=0, keepdims=True)
    before = jnp.sum(jnp.where(place == spot - 1, down, 0), axis=0, keepdims=True)
    before = jnp.where(lane == 0, -1, before // 4096)
    key = down // 4096
    last = jnp.sum((key <= spot).astype(jnp.int32), axis=0, keepdims=True) - 1
    has = jnp.sum((key == spot).astype(jnp.int32), axis=0, keepdims=True)
    keep = (here // 4096 == before).astype(jnp.int32)
    return here % 64, here // 64 % 64, keep, jnp.maximum(last, 0), jnp.minimum(has, 1)


def halves(value):
    high = value.astype(BF16)
    return high, (value - high.astype(F32)).astype(BF16)


def solve_kernel(
    depth, n_gx, n_gy, n_z,
    row_ref, col_ref, send_list, mass, moduli, guess, loads, tiles,
    sol, res,
    stage, tile, tile_t, hist, rhs, ext, stress, scan, own, strain0, norm0, coef,
    send_f, recv_f, send_r, recv_r, red_send, red_recv, table, tab, back_at, back_has,
    tile_sem, in_sem, tab_sem, fs_sem, fr_sem, rs_sem, rr_sem, ds_sem, dr_sem,
):
    slots, block = stage.shape[:2]
    blocks, rows = hist.shape[2:4]
    extent = blocks + 4 * depth
    groups = range(GROUPS)
    gx, gy = lax.axis_index("gx"), lax.axis_index("gy")
    n_y = n_gx // n_z
    y, z = gx // n_z, gx % n_z

    def chip(yy, zz):
        return yy * n_z + zz

    around = [
        ((gx + n_gx - 1) % n_gx, gy),
        ((gx + 1) % n_gx, gy),
        (gx, (gy + n_gy - 1) % n_gy),
        (gx, (gy + 1) % n_gy),
    ]
    phases = [
        [(gx, (gy + k) % n_gy) for k in range(1, n_gy)],
        [(chip((y + k) % n_y, z), gy) for k in range(1, n_y)],
        [(chip(y, (z + k) % n_z), gy) for k in range(1, n_z)],
    ]
    starts = [0, len(phases[0]), len(phases[0]) + len(phases[1])]

    barrier = pltpu.get_barrier_semaphore()
    greet = around[:2] + phases[0] + phases[1] + phases[2]
    for device in greet:
        pl.semaphore_signal(barrier, inc=1, device_id=device, device_id_type=MESH)

    def piece(whole, at, g, b, n):
        return pltpu.make_async_copy(
            whole.at[pl.ds(g * rows, rows), pl.ds(b * block, block)], at.at[g, b], in_sem.at[n, g, b]
        )

    for g in groups:
        for b in range(blocks):
            piece(guess, hist.at[0], g, b, 0).start()
    per = slots // CHUNKS
    loads_in = [
        pltpu.make_async_copy(tiles.at[pl.ds(c * per, per)], stage.at[pl.ds(c * per, per)], tile_sem.at[c])
        for c in range(CHUNKS)
    ]
    for copy in loads_in:
        copy.start()
    for g in groups:
        for b in range(blocks):
            piece(loads, rhs, g, b, 1).start()

    lane = lax.broadcasted_iota(jnp.int32, (1, 128), 1)
    row_of = jnp.full((1, 128), -2, jnp.int32)
    col_of = jnp.zeros((1, 128), jnp.int32)
    for t in range(slots):
        row_of = jnp.where(lane == t, row_ref[t], row_of)
        col_of = jnp.where(lane == t, col_ref[t], col_of)
    used, spare = row_of >= 0, (row_of < -1).astype(jnp.int32)
    by_row = sorted_slots(jnp.where(used, row_of, blocks + spare), col_of, lane)
    by_col = sorted_slots(jnp.where(used, col_of, extent + spare), jnp.maximum(row_of, 0), lane)
    for at, value in enumerate(by_row[:3] + by_col[:3] + (by_row[3],) + by_col[3:]):
        table[at : at + 1] = value
    for d in range(4):
        for b in range(blocks):
            at, has = jnp.int32(0), jnp.int32(0)
            for h in range(depth):
                same = send_list[0, d, h] == b
                at, has = jnp.where(same, h, at), jnp.where(same, 1, has)
            back_at[d * blocks + b] = at
            back_has[d * blocks + b] = has

    def listed(d, h):
        entry = send_list[0, d, h]
        return jnp.maximum(entry, 0), jnp.where(entry >= 0, 1.0, 0.0)

    def flag(at, t):
        return tab[at, t].astype(F32)

    def lanes(ref, b):
        return ref[b * block : (b + 1) * block].reshape(1, block)

    def forward(g, d):
        return pltpu.make_async_remote_copy(
            src_ref=send_f.at[g, d],
            dst_ref=recv_f.at[g, d ^ 1],
            send_sem=fs_sem.at[g, d],
            recv_sem=fr_sem.at[g, d ^ 1],
            device_id=around[d],
            device_id_type=MESH,
        )

    def backward(g, d):
        return pltpu.make_async_remote_copy(
            src_ref=send_r.at[g, d],
            dst_ref=recv_r[g].at[d ^ 1],
            send_sem=rs_sem.at[g, d],
            recv_sem=rr_sem.at[g, d ^ 1],
            device_id=around[d],
            device_id_type=MESH,
        )

    def wait_recv(make, g):
        for d in range(4):
            make(g, d ^ 1).wait_recv()

    def pack(step, g):
        for d in range(4):
            for h in range(depth):
                at, has = listed(d, h)
                send_f[g, d, h] = hist[step, g, at] * has

    def split_own(step, g):
        for b in range(blocks):
            high, low = halves(hist[step, g, b])
            ext[g, b, :rows] = high
            ext[g, b, rows:] = low

    def split_halo(g):
        for d in range(4):
            for h in range(depth):
                high, low = halves(recv_f[g, d, h])
                ext[g, blocks + d * depth + h, :rows] = high
                ext[g, blocks + d * depth + h, rows:] = low

    def sweep(source, g, weights, slot_at, block_at, keep_at):
        def body(i, total):
            for u in range(UNROLL):
                t = i * UNROLL + u
                x = source[g, tab[block_at, t]]
                both = jnp.dot(
                    jnp.concatenate([x, x], axis=1), weights[tab[slot_at, t]], preferred_element_type=F32
                )
                total = total * flag(keep_at, t) + (both[:rows] + both[rows:])
                scan[t] = total
            return total

        lax.fori_loop(0, slots // UNROLL, body, jnp.zeros((rows, block), F32))

    def strain_pass(step, g):
        sweep(ext, g, tile_t, ROW_SLOT, ROW_COL, ROW_KEEP)
        square = jnp.zeros((rows, block), F32)
        energy = jnp.zeros((rows, block), F32)
        if step == 2:
            norm, curve = reduce_end(0, g)
            norm0[g] = norm
            coef[g, 0] = norm / curve
            alpha = wide(norm / curve)
        for b in range(blocks):
            strain = scan[tab[ROW_LAST, b]]
            module = lanes(moduli, b)
            value = module * strain
            high, low = halves(value)
            stress[g, b, :rows] = high
            stress[g, b, rows:] = low
            if step == 1:
                strain0[g, b] = strain
                r = hist[1, g, b]
                square += r * r
                energy += value * strain + lanes(mass, b) * (r * r)
            if step == 2:
                r = hist[1, g, b] - alpha * hist[2, g, b]
                mixed = strain0[g, b] - alpha * strain
                square += r * r
                energy += module * (mixed * mixed) + lanes(mass, b) * (r * r)
        return square, energy

    def back_pass(step, g):
        sweep(stress, g, tile, COL_SLOT, COL_ROW, COL_KEEP)
        if step > 0:
            for d in range(4):
                backward(g, d).wait_send()
        for d in range(4):
            for h in range(depth):
                e = blocks + d * depth + h
                send_r[g, d, h] = scan[tab[COL_LAST, e]] * flag(COL_HAS, e)
        for d in range(4):
            backward(g, d).start()
        for b in range(blocks):
            own[g, b] = scan[tab[COL_LAST, b]] * flag(COL_HAS, b) + lanes(mass, b) * hist[step, g, b]

    def total_of(g, b):
        total = own[g, b]
        for d in range(4):
            k = d * blocks + b
            total += recv_r[g][d, back_at[k]] * back_has[k].astype(F32)
        return total

    def reduce_copies(which, g, phase):
        return [
            pltpu.make_async_remote_copy(
                src_ref=red_send.at[which, g, phase],
                dst_ref=red_recv.at[which, g, starts[phase] + i],
                send_sem=ds_sem.at[which, g, starts[phase] + i],
                recv_sem=dr_sem.at[which, g, starts[phase] + i],
                device_id=device,
                device_id_type=MESH,
            )
            for i, device in enumerate(phases[phase])
        ]

    def reduce_start(which, g, square, energy):
        half = block // 2
        stacked = jnp.concatenate(
            [
                square[:, :half] + square[:, half:],
                energy[:, :half] + energy[:, half:],
                jnp.zeros((128 - 2 * rows, half), F32),
            ],
            axis=0,
        )
        red_send[which, g, 0] = jnp.sum(stacked.T, axis=0, keepdims=True)
        for copy in reduce_copies(which, g, 0):
            copy.start()

    def reduced(which, g, phase):
        value = red_send[which, g, phase]
        for i, copy in enumerate(reduce_copies(which, g, phase)):
            copy.wait_recv()
            value += red_recv[which, g, starts[phase] + i]
        return value

    def reduce_next(which, g, phase):
        red_send[which, g, phase + 1] = reduced(which, g, phase)
        for copy in reduce_copies(which, g, phase + 1):
            copy.start()

    def reduce_end(which, g):
        spread = jnp.broadcast_to(reduced(which, g, 2), (128, 128)).T
        return spread[:rows], spread[rows : 2 * rows]

    def wide(value):
        return jnp.concatenate([value, value], axis=1)

    for g in groups:
        for b in range(blocks):
            piece(guess, hist.at[0], g, b, 0).wait()
    for g in groups:
        pack(0, g)
    pl.semaphore_wait(barrier, len(greet))
    for g in groups:
        for d in range(4):
            forward(g, d).start()
        split_own(0, g)
    to_smem = pltpu.make_async_copy(table, tab, tab_sem)
    to_smem.start()

    for c in range(CHUNKS):
        loads_in[c].wait()

        def split_tile(i, carry):
            t = c * per + i
            value = stage[t]
            high, low = halves(value)
            tile[t, :block] = high
            tile[t, block:] = low
            high, low = halves(value.T)
            tile_t[t, :block] = high
            tile_t[t, block:] = low
            return carry

        lax.fori_loop(0, per, split_tile, 0)

    def strain_half(step, g):
        wait_recv(forward, g)
        split_halo(g)
        square, energy = strain_pass(step, g)
        if step > 0:
            reduce_start(step - 1, g, square, energy)

    def finish(step, g):
        wait_recv(backward, g)
        for b in range(blocks):
            value = total_of(g, b)
            if step == 0:
                value = rhs[g, b] - value
            hist[step + 1, g, b] = value
        for d in range(4):
            forward(g, d).wait_send()
        pack(step + 1, g)
        for d in range(4):
            forward(g, d).start()
        split_own(step + 1, g)

    def last(g):
        wait_recv(backward, g)
        norm, curve = reduce_end(1, g)
        alpha0 = coef[g, 0]
        beta = norm / norm0[g]
        alpha1 = norm / (curve - beta * norm / alpha0)
        alpha0, alpha1, beta = wide(alpha0), wide(alpha1), wide(beta)
        for b in range(blocks):
            r0, w1 = hist[1, g, b], hist[2, g, b]
            w2 = total_of(g, b)
            r1 = r0 - alpha0 * w1
            part = (slice(g * rows, (g + 1) * rows), slice(b * block, (b + 1) * block))
            sol[part] = hist[0, g, b] + alpha0 * r0 + alpha1 * (r1 + beta * r0)
            res[part] = r1 - alpha1 * (w1 - alpha0 * w2 + beta * w1)

    to_smem.wait()
    for g in groups:
        for b in range(blocks):
            piece(loads, rhs, g, b, 1).wait()

    strain_half(0, 0)
    back_pass(0, 0)
    strain_half(0, 1)
    finish(0, 0)
    back_pass(0, 1)
    strain_half(1, 0)
    finish(0, 1)
    back_pass(1, 0)
    reduce_next(0, 0, 0)
    strain_half(1, 1)
    finish(1, 0)
    reduce_next(0, 0, 1)
    back_pass(1, 1)
    reduce_next(0, 1, 0)
    strain_half(2, 0)
    finish(1, 1)
    reduce_next(0, 1, 1)
    back_pass(2, 0)
    reduce_next(1, 0, 0)
    strain_half(2, 1)
    reduce_next(1, 0, 1)
    back_pass(2, 1)
    reduce_next(1, 1, 0)
    last(0)
    reduce_next(1, 1, 1)
    last(1)
    for g in groups:
        for d in range(4):
            forward(g, d).wait_send()
            backward(g, d).wait_send()
        for which in range(2):
            for phase in range(3):
                for copy in reduce_copies(which, g, phase):
                    copy.wait_send()


def solution(mesh):
    n_gx, n_gy = mesh.shape["gx"], mesh.shape["gy"]
    n_z = 8 if n_gx % 8 == 0 and n_gx > 8 else 2

    def on_device(loads, guess, mass, moduli, tiles, tile_row, tile_col, send_list):
        cases, width = loads.shape
        slots, block = tiles.shape[0], tiles.shape[1]
        depth = send_list.shape[2]
        blocks = width // block
        rows = cases // GROUPS
        extent = blocks + 4 * depth
        smem = pl.BlockSpec(memory_space=pltpu.SMEM)
        vmem = pl.BlockSpec(memory_space=pltpu.VMEM)
        hbm = pl.BlockSpec(memory_space=pl.ANY)
        peers = (n_gy - 1) + (n_gx // n_z - 1) + (n_z - 1)
        halo = (GROUPS, 4, depth, rows, block)
        dma = pltpu.SemaphoreType.DMA
        return pl.pallas_call(
            functools.partial(solve_kernel, depth, n_gx, n_gy, n_z),
            out_shape=[pltpu.VMEM((cases, width), F32)] * 2,
            in_specs=[smem, smem, smem, vmem, vmem, hbm, hbm, hbm],
            out_specs=[vmem, vmem],
            scratch_shapes=[
                pltpu.VMEM((slots, block, block), F32),
                pltpu.VMEM((slots, 2 * block, block), BF16),
                pltpu.VMEM((slots, 2 * block, block), BF16),
                pltpu.VMEM((3, GROUPS, blocks, rows, block), F32),
                pltpu.VMEM((GROUPS, blocks, rows, block), F32),
                pltpu.VMEM((GROUPS, extent, 2 * rows, block), BF16),
                pltpu.VMEM((GROUPS, blocks, 2 * rows, block), BF16),
                pltpu.VMEM((slots, rows, block), F32),
                pltpu.VMEM((GROUPS, blocks, rows, block), F32),
                pltpu.VMEM((GROUPS, blocks, rows, block), F32),
                pltpu.VMEM((GROUPS, rows, 128), F32),
                pltpu.VMEM((GROUPS, 1, rows, 128), F32),
                pltpu.VMEM(halo, F32),
                pltpu.VMEM(halo, F32),
                pltpu.VMEM(halo, F32),
                [pltpu.VMEM(halo[1:], F32)] * GROUPS,
                pltpu.VMEM((2, GROUPS, 3, 1, 128), F32),
                pltpu.VMEM((2, GROUPS, peers, 1, 128), F32),
                pltpu.VMEM((16, 128), jnp.int32),
                pltpu.SMEM((16, 128), jnp.int32),
                pltpu.SMEM((4 * blocks,), jnp.int32),
                pltpu.SMEM((4 * blocks,), jnp.int32),
                dma((CHUNKS,)),
                dma((2, GROUPS, blocks)),
                dma,
                dma((GROUPS, 4)),
                dma((GROUPS, 4)),
                dma((GROUPS, 4)),
                dma((GROUPS, 4)),
                dma((2, GROUPS, peers)),
                dma((2, GROUPS, peers)),
            ],
            compiler_params=pltpu.CompilerParams(
                collective_id=0, has_side_effects=True, vmem_limit_bytes=60 * 1024 * 1024
            ),
            name="solve",
        )(tile_row, tile_col, send_list, mass, moduli, guess, loads, tiles)

    both = ("gx", "gy")
    return jax.shard_map(
        on_device,
        mesh=mesh,
        in_specs=(
            P(None, both), P(None, both), P(both), P(both), P(both, None, None), P(both), P(both), P(both, None, None),
        ),
        out_specs=(P(None, both), P(None, both)),
        check_vma=False,
    )
```

```python
import functools

import jax
import jax.numpy as jnp
from jax import lax
from jax.experimental import pallas as pl
from jax.experimental.pallas import tpu as pltpu
from jax.sharding import PartitionSpec as P

MESH = pl.DeviceIdType.MESH
GROUPS = 4
LAG = 2
CHUNKS = 8
UNROLL = 20
F32 = jnp.float32
BF16 = jnp.bfloat16
F8 = jnp.float8_e4m3fn
LOW_SCALE = 2.0**19


def tile_parts(value):
    high = value.astype(BF16)
    return high, ((value - high.astype(F32)) * LOW_SCALE).astype(F8)


ROW_SLOT, ROW_COL, ROW_KEEP, COL_SLOT, COL_ROW, COL_KEEP, ROW_LAST, COL_LAST, COL_HAS = range(9)


def sorted_slots(key_of, other, lane):
    code = (key_of * 64 + other) * 64 + lane
    across = jnp.broadcast_to(code, (128, 128))
    down = across.T
    place = jnp.sum((down < across).astype(jnp.int32), axis=0, keepdims=True)
    place = jnp.broadcast_to(place, (128, 128)).T
    spot = jnp.broadcast_to(lane, (128, 128))
    here = jnp.sum(jnp.where(place == spot, down, 0), axis=0, keepdims=True)
    before = jnp.sum(jnp.where(place == spot - 1, down, 0), axis=0, keepdims=True)
    before = jnp.where(lane == 0, -1, before // 4096)
    key = down // 4096
    last = jnp.sum((key <= spot).astype(jnp.int32), axis=0, keepdims=True) - 1
    has = jnp.sum((key == spot).astype(jnp.int32), axis=0, keepdims=True)
    keep = (here // 4096 == before).astype(jnp.int32)
    return here % 64, here // 64 % 64, keep, jnp.maximum(last, 0), jnp.minimum(has, 1)


def halves(value):
    high = value.astype(BF16)
    return high, (value - high.astype(F32)).astype(BF16)


def solve_kernel(
    depth, n_gx, n_gy, n_z,
    row_ref, col_ref, send_list, mass, moduli, guess, loads, tiles,
    sol, res,
    stage, tile, tile_low, tile_t, tile_t_low, hist, rhs, ext, stress, scan, own, strain0, norm0, coef,
    send_f, recv_f, send_r, recv_r, red_send, red_recv, table, tab, back_at, back_has,
    tile_sem, in_sem, tab_sem, fs_sem, fr_sem, rs_sem, rr_sem, ds_sem, dr_sem,
):
    slots, block = stage.shape[:2]
    blocks, rows = hist.shape[2:4]
    extent = blocks + 4 * depth
    groups = range(GROUPS)
    gx, gy = lax.axis_index("gx"), lax.axis_index("gy")
    n_y = n_gx // n_z
    y, z = gx // n_z, gx % n_z

    def chip(yy, zz):
        return yy * n_z + zz

    around = [
        ((gx + n_gx - 1) % n_gx, gy),
        ((gx + 1) % n_gx, gy),
        (gx, (gy + n_gy - 1) % n_gy),
        (gx, (gy + 1) % n_gy),
    ]
    there = [gx > 0, gx < n_gx - 1, gy > 0, gy < n_gy - 1]
    phases = [
        [(gx, (gy + k) % n_gy) for k in range(1, n_gy)],
        [(chip((y + k) % n_y, z), gy) for k in range(1, n_y)],
        [(chip(y, (z + k) % n_z), gy) for k in range(1, n_z)],
    ]
    starts = [0, len(phases[0]), len(phases[0]) + len(phases[1])]

    barrier = pltpu.get_barrier_semaphore()
    greet = around[:2] + phases[0] + phases[1] + phases[2]
    for device in greet:
        pl.semaphore_signal(barrier, inc=1, device_id=device, device_id_type=MESH)

    def piece(whole, at, g, b, n):
        return pltpu.make_async_copy(
            whole.at[pl.ds(g * rows, rows), pl.ds(b * block, block)], at.at[g, b], in_sem.at[n, g, b]
        )

    for g in groups:
        for b in range(blocks):
            piece(guess, hist.at[0], g, b, 0).start()
    per = slots // CHUNKS
    loads_in = [
        pltpu.make_async_copy(tiles.at[pl.ds(c * per, per)], stage.at[pl.ds(c * per, per)], tile_sem.at[c])
        for c in range(CHUNKS)
    ]
    for copy in loads_in:
        copy.start()
    for g in groups:
        for b in range(blocks):
            piece(loads, rhs, g, b, 1).start()

    lane = lax.broadcasted_iota(jnp.int32, (1, 128), 1)
    row_of = jnp.full((1, 128), -2, jnp.int32)
    col_of = jnp.zeros((1, 128), jnp.int32)
    for t in range(slots):
        row_of = jnp.where(lane == t, row_ref[t], row_of)
        col_of = jnp.where(lane == t, col_ref[t], col_of)
    used, spare = row_of >= 0, (row_of < -1).astype(jnp.int32)
    by_row = sorted_slots(jnp.where(used, row_of, blocks + spare), col_of, lane)
    by_col = sorted_slots(jnp.where(used, col_of, extent + spare), jnp.maximum(row_of, 0), lane)
    for at, value in enumerate(by_row[:3] + by_col[:3] + (by_row[3],) + by_col[3:]):
        table[at : at + 1] = value
    for d in range(4):
        for b in range(blocks):
            at, has = jnp.int32(0), jnp.int32(0)
            for h in range(depth):
                same = send_list[0, d, h] == b
                at, has = jnp.where(same, h, at), jnp.where(same, 1, has)
            back_at[d * blocks + b] = at
            back_has[d * blocks + b] = has

    def listed(d, h):
        entry = send_list[0, d, h]
        return jnp.maximum(entry, 0), jnp.where(entry >= 0, 1.0, 0.0)

    def flag(at, t):
        return tab[at, t].astype(F32)

    def lanes(ref, b):
        return ref[b * block : (b + 1) * block].reshape(1, block)

    def forward(g, d):
        return pltpu.make_async_remote_copy(
            src_ref=send_f.at[g, d],
            dst_ref=recv_f.at[g, d ^ 1],
            send_sem=fs_sem.at[g, d],
            recv_sem=fr_sem.at[g, d ^ 1],
            device_id=around[d],
            device_id_type=MESH,
        )

    def backward(g, d):
        return pltpu.make_async_remote_copy(
            src_ref=send_r.at[g, d],
            dst_ref=recv_r[g].at[d ^ 1],
            send_sem=rs_sem.at[g, d],
            recv_sem=rr_sem.at[g, d ^ 1],
            device_id=around[d],
            device_id_type=MESH,
        )

    def start(make, g):
        for d in range(4):
            pl.when(there[d])(make(g, d).start)

    def wait_send(make, g):
        for d in range(4):
            pl.when(there[d])(make(g, d).wait_send)

    def wait_recv(make, g):
        for d in range(4):
            pl.when(there[d])(make(g, d ^ 1).wait_recv)

    def pack(step, g):
        for d in range(4):
            for h in range(depth):
                at, has = listed(d, h)
                send_f[g, d, h] = hist[step, g, at] * has

    def split_own(step, g):
        for b in range(blocks):
            high, low = halves(hist[step, g, b])
            ext[g, b, :rows] = high
            ext[g, b, rows:] = low

    def split_halo(g):
        for d in range(4):
            for h in range(depth):
                high, low = halves(recv_f[g, d, h])
                ext[g, blocks + d * depth + h, :rows] = high
                ext[g, blocks + d * depth + h, rows:] = low

    def sweep(source, g, high, low, slot_at, block_at, keep_at):
        def body(i, total):
            for u in range(UNROLL):
                t = i * UNROLL + u
                x = source[g, tab[block_at, t]]
                slot = tab[slot_at, t]
                both = jnp.dot(x, high[slot], preferred_element_type=F32)
                rest = jnp.dot(x[:rows], low[slot], preferred_element_type=F32)
                both = both[:rows] + both[rows:] + rest * (1.0 / LOW_SCALE)
                total = total * flag(keep_at, t) + both
                scan[t] = total
            return total

        lax.fori_loop(0, slots // UNROLL, body, jnp.zeros((rows, block), F32))

    def strain_pass(step, g):
        sweep(ext, g, tile_t, tile_t_low, ROW_SLOT, ROW_COL, ROW_KEEP)
        square = jnp.zeros((rows, block), F32)
        energy = jnp.zeros((rows, block), F32)
        if step == 2:
            norm, curve = reduce_end(0, g)
            norm0[g] = norm
            coef[g, 0] = norm / curve
            alpha = wide(norm / curve)
        for b in range(blocks):
            strain = scan[tab[ROW_LAST, b]]
            module = lanes(moduli, b)
            value = module * strain
            high, low = halves(value)
            stress[g, b, :rows] = high
            stress[g, b, rows:] = low
            if step == 1:
                strain0[g, b] = strain
                r = hist[1, g, b]
                square += r * r
                energy += value * strain + lanes(mass, b) * (r * r)
            if step == 2:
                r = hist[1, g, b] - alpha * hist[2, g, b]
                mixed = strain0[g, b] - alpha * strain
                square += r * r
                energy += module * (mixed * mixed) + lanes(mass, b) * (r * r)
        return square, energy

    def back_pass(step, g):
        sweep(stress, g, tile, tile_low, COL_SLOT, COL_ROW, COL_KEEP)
        if step > 0:
            wait_send(backward, g)
        for d in range(4):
            for h in range(depth):
                e = blocks + d * depth + h
                send_r[g, d, h] = scan[tab[COL_LAST, e]] * flag(COL_HAS, e)
        start(backward, g)
        for b in range(blocks):
            own[g, b] = scan[tab[COL_LAST, b]] * flag(COL_HAS, b) + lanes(mass, b) * hist[step, g, b]

    def total_of(g, b):
        total = own[g, b]
        for d in range(4):
            k = d * blocks + b
            total += recv_r[g][d, back_at[k]] * back_has[k].astype(F32)
        return total

    def reduce_copies(which, g, phase):
        return [
            pltpu.make_async_remote_copy(
                src_ref=red_send.at[which, g, phase],
                dst_ref=red_recv.at[which, g, starts[phase] + i],
                send_sem=ds_sem.at[which, g, starts[phase] + i],
                recv_sem=dr_sem.at[which, g, starts[phase] + i],
                device_id=device,
                device_id_type=MESH,
            )
            for i, device in enumerate(phases[phase])
        ]

    def reduce_start(which, g, square, energy):
        half = block // 2
        stacked = jnp.concatenate(
            [
                square[:, :half] + square[:, half:],
                energy[:, :half] + energy[:, half:],
                jnp.zeros((128 - 2 * rows, half), F32),
            ],
            axis=0,
        )
        red_send[which, g, 0] = jnp.sum(stacked.T, axis=0, keepdims=True)
        for copy in reduce_copies(which, g, 0):
            copy.start()

    def reduced(which, g, phase):
        value = red_send[which, g, phase]
        for i, copy in enumerate(reduce_copies(which, g, phase)):
            copy.wait_recv()
            value += red_recv[which, g, starts[phase] + i]
        return value

    def reduce_next(which, g, phase):
        red_send[which, g, phase + 1] = reduced(which, g, phase)
        for copy in reduce_copies(which, g, phase + 1):
            copy.start()

    def reduce_end(which, g):
        spread = jnp.broadcast_to(reduced(which, g, 2), (128, 128)).T
        return spread[:rows], spread[rows : 2 * rows]

    def wide(value):
        return jnp.concatenate([value, value], axis=1)

    for g in groups:
        for b in range(blocks):
            piece(guess, hist.at[0], g, b, 0).wait()
    for g in groups:
        pack(0, g)
    for d in range(4):

        @pl.when(jnp.logical_not(there[d]))
        def _():
            for g in groups:
                recv_f[g, d] = jnp.zeros_like(recv_f[g, d])
                recv_r[g][d] = jnp.zeros_like(recv_r[g][d])

    pl.semaphore_wait(barrier, len(greet))
    for g in groups:
        start(forward, g)
        split_own(0, g)
    to_smem = pltpu.make_async_copy(table, tab, tab_sem)
    to_smem.start()

    for c in range(CHUNKS):
        loads_in[c].wait()

        def split_tile(i, carry):
            t = c * per + i
            value = stage[t]
            tile[t], tile_low[t] = tile_parts(value)
            tile_t[t], tile_t_low[t] = tile_parts(value.T)
            return carry

        lax.fori_loop(0, per, split_tile, 0)

    def strain_half(step, g):
        wait_recv(forward, g)
        split_halo(g)
        square, energy = strain_pass(step, g)
        if step > 0:
            reduce_start(step - 1, g, square, energy)

    def finish(step, g):
        wait_recv(backward, g)
        for b in range(blocks):
            value = total_of(g, b)
            if step == 0:
                value = rhs[g, b] - value
            hist[step + 1, g, b] = value
        wait_send(forward, g)
        pack(step + 1, g)
        start(forward, g)
        split_own(step + 1, g)

    def last(g):
        wait_recv(backward, g)
        norm, curve = reduce_end(1, g)
        alpha0 = coef[g, 0]
        beta = norm / norm0[g]
        alpha1 = norm / (curve - beta * norm / alpha0)
        alpha0, alpha1, beta = wide(alpha0), wide(alpha1), wide(beta)
        for b in range(blocks):
            r0, w1 = hist[1, g, b], hist[2, g, b]
            w2 = total_of(g, b)
            r1 = r0 - alpha0 * w1
            part = (slice(g * rows, (g + 1) * rows), slice(b * block, (b + 1) * block))
            sol[part] = hist[0, g, b] + alpha0 * r0 + alpha1 * (r1 + beta * r0)
            res[part] = r1 - alpha1 * (w1 - alpha0 * w2 + beta * w1)

    to_smem.wait()
    for g in groups:
        for b in range(blocks):
            piece(loads, rhs, g, b, 1).wait()

    turns = [(step, g) for step in range(3) for g in groups]
    for q, (step, g) in enumerate(turns):
        strain_half(step, g)
        if q >= LAG and turns[q - LAG][0] < 2:
            finish(*turns[q - LAG])
        for ago, phase in ((2, 1), (1, 0)) if GROUPS > 2 else ((1, 1),):
            if q >= ago and turns[q - ago][0] > 0:
                reduce_next(turns[q - ago][0] - 1, turns[q - ago][1], phase)
        back_pass(step, g)
        if GROUPS == 2 and step > 0:
            reduce_next(step - 1, g, 0)
    if GROUPS > 2:
        reduce_next(1, GROUPS - 1, 0)
        reduce_next(1, GROUPS - 2, 1)
    last(0)
    reduce_next(1, GROUPS - 1, 1)
    for g in groups[1:]:
        last(g)
    for g in groups:
        wait_send(forward, g)
        wait_send(backward, g)
        for which in range(2):
            for phase in range(3):
                for copy in reduce_copies(which, g, phase):
                    copy.wait_send()


def solution(mesh):
    n_gx, n_gy = mesh.shape["gx"], mesh.shape["gy"]
    n_z = 8 if n_gx % 8 == 0 and n_gx > 8 else 2

    def on_device(loads, guess, mass, moduli, tiles, tile_row, tile_col, send_list):
        cases, width = loads.shape
        slots, block = tiles.shape[0], tiles.shape[1]
        depth = send_list.shape[2]
        blocks = width // block
        rows = cases // GROUPS
        extent = blocks + 4 * depth
        smem = pl.BlockSpec(memory_space=pltpu.SMEM)
        vmem = pl.BlockSpec(memory_space=pltpu.VMEM)
        hbm = pl.BlockSpec(memory_space=pl.ANY)
        peers = (n_gy - 1) + (n_gx // n_z - 1) + (n_z - 1)
        halo = (GROUPS, 4, depth, rows, block)
        dma = pltpu.SemaphoreType.DMA
        return pl.pallas_call(
            functools.partial(solve_kernel, depth, n_gx, n_gy, n_z),
            out_shape=[pltpu.VMEM((cases, width), F32)] * 2,
            in_specs=[smem, smem, smem, vmem, vmem, hbm, hbm, hbm],
            out_specs=[vmem, vmem],
            scratch_shapes=[
                pltpu.VMEM((slots, block, block), F32),
                pltpu.VMEM((slots, block, block), BF16),
                pltpu.VMEM((slots, block, block), F8),
                pltpu.VMEM((slots, block, block), BF16),
                pltpu.VMEM((slots, block, block), F8),
                pltpu.VMEM((3, GROUPS, blocks, rows, block), F32),
                pltpu.VMEM((GROUPS, blocks, rows, block), F32),
                pltpu.VMEM((GROUPS, extent, 2 * rows, block), BF16),
                pltpu.VMEM((GROUPS, blocks, 2 * rows, block), BF16),
                pltpu.VMEM((slots, rows, block), F32),
                pltpu.VMEM((GROUPS, blocks, rows, block), F32),
                pltpu.VMEM((GROUPS, blocks, rows, block), F32),
                pltpu.VMEM((GROUPS, rows, 128), F32),
                pltpu.VMEM((GROUPS, 1, rows, 128), F32),
                pltpu.VMEM(halo, F32),
                pltpu.VMEM(halo, F32),
                pltpu.VMEM(halo, F32),
                [pltpu.VMEM(halo[1:], F32)] * GROUPS,
                pltpu.VMEM((2, GROUPS, 3, 1, 128), F32),
                pltpu.VMEM((2, GROUPS, peers, 1, 128), F32),
                pltpu.VMEM((16, 128), jnp.int32),
                pltpu.SMEM((16, 128), jnp.int32),
                pltpu.SMEM((4 * blocks,), jnp.int32),
                pltpu.SMEM((4 * blocks,), jnp.int32),
                dma((CHUNKS,)),
                dma((2, GROUPS, blocks)),
                dma,
                dma((GROUPS, 4)),
                dma((GROUPS, 4)),
                dma((GROUPS, 4)),
                dma((GROUPS, 4)),
                dma((2, GROUPS, peers)),
                dma((2, GROUPS, peers)),
            ],
            compiler_params=pltpu.CompilerParams(
                collective_id=0, has_side_effects=True, vmem_limit_bytes=60 * 1024 * 1024
            ),
            name="solve",
        )(tile_row, tile_col, send_list, mass, moduli, guess, loads, tiles)

    both = ("gx", "gy")
    return jax.shard_map(
        on_device,
        mesh=mesh,
        in_specs=(
            P(None, both), P(None, both), P(both), P(both), P(both, None, None), P(both), P(both), P(both, None, None),
        ),
        out_specs=(P(None, both), P(None, both)),
        check_vma=False,
    )
```

```python
import functools

import jax
import jax.numpy as jnp
from jax import lax
from jax.experimental import pallas as pl
from jax.experimental.pallas import tpu as pltpu
from jax.sharding import PartitionSpec as P

MESH = pl.DeviceIdType.MESH
GROUPS = 4
LAG = 2
PIECES = 1
EARLY = 3
CHUNKS = 8
UNROLL = 40
F32 = jnp.float32
BF16 = jnp.bfloat16
F8 = jnp.float8_e4m3fn
LOW_SCALE = 2.0**19


def tile_parts(value):
    high = value.astype(BF16)
    return high, ((value - high.astype(F32)) * LOW_SCALE).astype(F8)


ROW_SLOT, ROW_COL, ROW_KEEP, COL_SLOT, COL_ROW, COL_KEEP, ROW_LAST, COL_LAST, COL_HAS = range(9)


def sorted_slots(key_of, other, lane):
    code = (key_of * 64 + other) * 64 + lane
    across = jnp.broadcast_to(code, (128, 128))
    down = across.T
    place = jnp.sum((down < across).astype(jnp.int32), axis=0, keepdims=True)
    place = jnp.broadcast_to(place, (128, 128)).T
    spot = jnp.broadcast_to(lane, (128, 128))
    here = jnp.sum(jnp.where(place == spot, down, 0), axis=0, keepdims=True)
    before = jnp.sum(jnp.where(place == spot - 1, down, 0), axis=0, keepdims=True)
    before = jnp.where(lane == 0, -1, before // 4096)
    key = down // 4096
    last = jnp.sum((key <= spot).astype(jnp.int32), axis=0, keepdims=True) - 1
    has = jnp.sum((key == spot).astype(jnp.int32), axis=0, keepdims=True)
    keep = (here // 4096 == before).astype(jnp.int32)
    return here % 64, here // 64 % 64, keep, jnp.maximum(last, 0), jnp.minimum(has, 1)


def halves(value):
    high = value.astype(BF16)
    return high, (value - high.astype(F32)).astype(BF16)


def solve_kernel(
    depth, n_gx, n_gy, n_z,
    row_ref, col_ref, send_list, mass, moduli, guess, loads, tiles,
    sol, res,
    stage, tile, tile_low, tile_t, tile_t_low, hist, rhs, ext, stress, scan, own, strain0, norm0, coef,
    send_f, recv_f, send_r, recv_r, red_send, red_recv, table, tab, back_at, back_has,
    tile_sem, in_sem, tab_sem, fs_sem, fr_sem, rs_sem, rr_sem, ds_sem, dr_sem,
):
    slots, block = stage.shape[:2]
    blocks, rows = hist.shape[2:4]
    extent = blocks + 4 * depth
    groups = range(GROUPS)
    pieces = [(p, pl.ds(p * (rows // PIECES), rows // PIECES)) for p in range(PIECES)]
    gx, gy = lax.axis_index("gx"), lax.axis_index("gy")
    n_y = n_gx // n_z
    y, z = gx // n_z, gx % n_z

    def chip(yy, zz):
        return yy * n_z + zz

    around = [
        ((gx + n_gx - 1) % n_gx, gy),
        ((gx + 1) % n_gx, gy),
        (gx, (gy + n_gy - 1) % n_gy),
        (gx, (gy + 1) % n_gy),
    ]
    there = [gx > 0, gx < n_gx - 1, gy > 0, gy < n_gy - 1]
    phases = [
        [(gx, (gy + k) % n_gy) for k in range(1, n_gy)],
        [(chip((y + k) % n_y, z), gy) for k in range(1, n_y)],
        [(chip(y, (z + k) % n_z), gy) for k in range(1, n_z)],
    ]
    starts = [0, len(phases[0]), len(phases[0]) + len(phases[1])]

    barrier = pltpu.get_barrier_semaphore()
    greet = around[:2] + phases[0] + phases[1] + phases[2]
    for device in greet:
        pl.semaphore_signal(barrier, inc=1, device_id=device, device_id_type=MESH)

    def piece(whole, at, g, b, n):
        return pltpu.make_async_copy(
            whole.at[pl.ds(g * rows, rows), pl.ds(b * block, block)], at.at[g, b], in_sem.at[n, g, b]
        )

    for g in groups:
        for b in range(blocks):
            piece(guess, hist.at[0], g, b, 0).start()
    per = slots // CHUNKS
    loads_in = [
        pltpu.make_async_copy(tiles.at[pl.ds(c * per, per)], stage.at[pl.ds(c * per, per)], tile_sem.at[c])
        for c in range(CHUNKS)
    ]
    for copy in loads_in:
        copy.start()
    for g in groups:
        for b in range(blocks):
            piece(loads, rhs, g, b, 1).start()

    lane = lax.broadcasted_iota(jnp.int32, (1, 128), 1)
    row_of = jnp.full((1, 128), -2, jnp.int32)
    col_of = jnp.zeros((1, 128), jnp.int32)
    for t in range(slots):
        row_of = jnp.where(lane == t, row_ref[t], row_of)
        col_of = jnp.where(lane == t, col_ref[t], col_of)
    used, spare = row_of >= 0, (row_of < -1).astype(jnp.int32)
    by_row = sorted_slots(jnp.where(used, row_of, blocks + spare), col_of, lane)
    by_col = sorted_slots(jnp.where(used, col_of, extent + spare), jnp.maximum(row_of, 0), lane)
    for at, value in enumerate(by_row[:3] + by_col[:3] + (by_row[3],) + by_col[3:]):
        table[at : at + 1] = value
    for d in range(4):
        for b in range(blocks):
            at, has = jnp.int32(0), jnp.int32(0)
            for h in range(depth):
                same = send_list[0, d, h] == b
                at, has = jnp.where(same, h, at), jnp.where(same, 1, has)
            back_at[d * blocks + b] = at
            back_has[d * blocks + b] = has

    def listed(d, h):
        entry = send_list[0, d, h]
        return jnp.maximum(entry, 0), jnp.where(entry >= 0, 1.0, 0.0)

    def flag(at, t):
        return tab[at, t].astype(F32)

    def lanes(ref, b):
        return ref[b * block : (b + 1) * block].reshape(1, block)

    def forward(g, p, d):
        return pltpu.make_async_remote_copy(
            src_ref=send_f.at[g, p, d],
            dst_ref=recv_f.at[g, p, d ^ 1],
            send_sem=fs_sem.at[g, p, d],
            recv_sem=fr_sem.at[g, p, d ^ 1],
            device_id=around[d],
            device_id_type=MESH,
        )

    def backward(g, p, d):
        return pltpu.make_async_remote_copy(
            src_ref=send_r.at[g, p, d],
            dst_ref=recv_r[g][p].at[d ^ 1],
            send_sem=rs_sem.at[g, p, d],
            recv_sem=rr_sem.at[g, p, d ^ 1],
            device_id=around[d],
            device_id_type=MESH,
        )

    def start(make, g, p):
        for d in range(4):
            pl.when(there[d])(make(g, p, d).start)

    def wait_send(make, g, p):
        for d in range(4):
            pl.when(there[d])(make(g, p, d).wait_send)

    def wait_recv(make, g, p):
        for d in range(4):
            pl.when(there[d])(make(g, p, d ^ 1).wait_recv)

    def pack(step, g, p, part):
        for d in range(4):
            for h in range(depth):
                at, has = listed(d, h)
                send_f[g, p, d, h] = hist[step, g, at, part] * has

    def split_own(step, g):
        for b in range(blocks):
            high, low = halves(hist[step, g, b])
            ext[g, b, :rows] = high
            ext[g, b, rows:] = low

    def split_halo(g, p, part):
        for d in range(4):
            for h in range(depth):
                high, low = halves(recv_f[g, p, d, h])
                ext[g, blocks + d * depth + h, part] = high
                ext[g, blocks + d * depth + h, pl.ds(rows + part.start, part.size)] = low

    def sweep(source, g, high, low, slot_at, block_at, keep_at):
        def body(i, total):
            for u in range(UNROLL):
                t = i * UNROLL + u
                x = source[g, tab[block_at, t]]
                slot = tab[slot_at, t]
                both = jnp.dot(x, high[slot], preferred_element_type=F32)
                rest = jnp.dot(x[:rows], low[slot], preferred_element_type=F32)
                both = both[:rows] + both[rows:] + rest * (1.0 / LOW_SCALE)
                total = total * flag(keep_at, t) + both
                scan[t] = total
            return total

        lax.fori_loop(0, slots // UNROLL, body, jnp.zeros((rows, block), F32))

    def strain_pass(step, g):
        sweep(ext, g, tile_t, tile_t_low, ROW_SLOT, ROW_COL, ROW_KEEP)
        square = jnp.zeros((rows, block), F32)
        energy = jnp.zeros((rows, block), F32)
        if step == 2:
            norm, curve = reduce_end(0, g)
            norm0[g] = norm
            coef[g, 0] = norm / curve
            alpha = wide(norm / curve)
        for b in range(blocks):
            strain = scan[tab[ROW_LAST, b]]
            module = lanes(moduli, b)
            value = module * strain
            high, low = halves(value)
            stress[g, b, :rows] = high
            stress[g, b, rows:] = low
            if step == 1:
                strain0[g, b] = strain
                r = hist[1, g, b]
                square += r * r
                energy += value * strain + lanes(mass, b) * (r * r)
            if step == 2:
                r = hist[1, g, b] - alpha * hist[2, g, b]
                mixed = strain0[g, b] - alpha * strain
                square += r * r
                energy += module * (mixed * mixed) + lanes(mass, b) * (r * r)
        return square, energy

    def back_pass(step, g):
        sweep(stress, g, tile, tile_low, COL_SLOT, COL_ROW, COL_KEEP)
        for p, part in pieces:
            if step > 0:
                wait_send(backward, g, p)
            for d in range(4):
                for h in range(depth):
                    e = blocks + d * depth + h
                    send_r[g, p, d, h] = scan[tab[COL_LAST, e], part] * flag(COL_HAS, e)
            start(backward, g, p)
        for b in range(blocks):
            own[g, b] = scan[tab[COL_LAST, b]] * flag(COL_HAS, b) + lanes(mass, b) * hist[step, g, b]

    def total_of(g, b, p, part):
        total = own[g, b, part]
        for d in range(4):
            k = d * blocks + b
            total += recv_r[g][p][d, back_at[k]] * back_has[k].astype(F32)
        return total

    def reduce_copies(which, g, phase):
        return [
            pltpu.make_async_remote_copy(
                src_ref=red_send.at[which, g, phase],
                dst_ref=red_recv.at[which, g, starts[phase] + i],
                send_sem=ds_sem.at[which, g, starts[phase] + i],
                recv_sem=dr_sem.at[which, g, starts[phase] + i],
                device_id=device,
                device_id_type=MESH,
            )
            for i, device in enumerate(phases[phase])
        ]

    def reduce_start(which, g, square, energy):
        half = block // 2
        stacked = jnp.concatenate(
            [
                square[:, :half] + square[:, half:],
                energy[:, :half] + energy[:, half:],
                jnp.zeros((128 - 2 * rows, half), F32),
            ],
            axis=0,
        )
        red_send[which, g, 0] = jnp.sum(stacked.T, axis=0, keepdims=True)
        for copy in reduce_copies(which, g, 0):
            copy.start()

    def reduced(which, g, phase):
        value = red_send[which, g, phase]
        for i, copy in enumerate(reduce_copies(which, g, phase)):
            copy.wait_recv()
            value += red_recv[which, g, starts[phase] + i]
        return value

    def reduce_next(which, g, phase):
        red_send[which, g, phase + 1] = reduced(which, g, phase)
        for copy in reduce_copies(which, g, phase + 1):
            copy.start()

    def reduce_end(which, g):
        spread = jnp.broadcast_to(reduced(which, g, 2), (128, 128)).T
        return spread[:rows], spread[rows : 2 * rows]

    def wide(value):
        return jnp.concatenate([value, value], axis=1)

    for g in groups:
        for b in range(blocks):
            piece(guess, hist.at[0], g, b, 0).wait()
    for g in groups:
        for p, part in pieces:
            pack(0, g, p, part)
    for d in range(4):

        @pl.when(jnp.logical_not(there[d]))
        def _():
            for g in groups:
                for p in range(PIECES):
                    recv_f[g, p, d] = jnp.zeros_like(recv_f[g, p, d])
                    recv_r[g][p][d] = jnp.zeros_like(recv_r[g][p][d])

    def split_chunk(c):
        loads_in[c].wait()

        def split_tile(i, carry):
            t = c * per + i
            value = stage[t]
            tile[t], tile_low[t] = tile_parts(value)
            tile_t[t], tile_t_low[t] = tile_parts(value.T)
            return carry

        lax.fori_loop(0, per, split_tile, 0)

    for c in range(EARLY):
        split_chunk(c)
    pl.semaphore_wait(barrier, len(greet))
    for g in groups:
        for p, _ in pieces:
            start(forward, g, p)
        split_own(0, g)
    to_smem = pltpu.make_async_copy(table, tab, tab_sem)
    to_smem.start()
    for c in range(EARLY, CHUNKS):
        split_chunk(c)

    def strain_half(step, g):
        for p, part in pieces:
            wait_recv(forward, g, p)
            split_halo(g, p, part)
        square, energy = strain_pass(step, g)
        if step > 0:
            reduce_start(step - 1, g, square, energy)

    def finish(step, g):
        for p, part in pieces:
            wait_recv(backward, g, p)
            for b in range(blocks):
                value = total_of(g, b, p, part)
                if step == 0:
                    value = rhs[g, b, part] - value
                hist[step + 1, g, b, part] = value
            wait_send(forward, g, p)
            pack(step + 1, g, p, part)
            start(forward, g, p)
        split_own(step + 1, g)

    def last(g):
        for p, _ in pieces:
            wait_recv(backward, g, p)
        norm, curve = reduce_end(1, g)
        alpha0 = coef[g, 0]
        beta = norm / norm0[g]
        alpha1 = norm / (curve - beta * norm / alpha0)
        alpha0, alpha1, beta = wide(alpha0), wide(alpha1), wide(beta)
        for b in range(blocks):
            r0, w1 = hist[1, g, b], hist[2, g, b]
            w2 = jnp.concatenate([total_of(g, b, p, part) for p, part in pieces], axis=0)
            r1 = r0 - alpha0 * w1
            place = (slice(g * rows, (g + 1) * rows), slice(b * block, (b + 1) * block))
            sol[place] = hist[0, g, b] + alpha0 * r0 + alpha1 * (r1 + beta * r0)
            res[place] = r1 - alpha1 * (w1 - alpha0 * w2 + beta * w1)

    to_smem.wait()
    for g in groups:
        for b in range(blocks):
            piece(loads, rhs, g, b, 1).wait()

    turns = [(step, g) for step in range(3) for g in groups]
    for q, (step, g) in enumerate(turns):
        strain_half(step, g)
        if q >= LAG and turns[q - LAG][0] < 2:
            finish(*turns[q - LAG])
        for ago, phase in ((2, 1), (1, 0)) if GROUPS > 2 else ((1, 1),):
            if q >= ago and turns[q - ago][0] > 0:
                reduce_next(turns[q - ago][0] - 1, turns[q - ago][1], phase)
        back_pass(step, g)
        if GROUPS == 2 and step > 0:
            reduce_next(step - 1, g, 0)
    if GROUPS > 2:
        reduce_next(1, GROUPS - 1, 0)
        reduce_next(1, GROUPS - 2, 1)
    last(0)
    reduce_next(1, GROUPS - 1, 1)
    for g in groups[1:]:
        last(g)
    for g in groups:
        for p, _ in pieces:
            wait_send(forward, g, p)
            wait_send(backward, g, p)
        for which in range(2):
            for phase in range(3):
                for copy in reduce_copies(which, g, phase):
                    copy.wait_send()


def solution(mesh):
    n_gx, n_gy = mesh.shape["gx"], mesh.shape["gy"]
    n_z = 8 if n_gx % 8 == 0 and n_gx > 8 else 2

    def on_device(loads, guess, mass, moduli, tiles, tile_row, tile_col, send_list):
        cases, width = loads.shape
        slots, block = tiles.shape[0], tiles.shape[1]
        depth = send_list.shape[2]
        blocks = width // block
        rows = cases // GROUPS
        extent = blocks + 4 * depth
        smem = pl.BlockSpec(memory_space=pltpu.SMEM)
        vmem = pl.BlockSpec(memory_space=pltpu.VMEM)
        hbm = pl.BlockSpec(memory_space=pl.ANY)
        peers = (n_gy - 1) + (n_gx // n_z - 1) + (n_z - 1)
        halo = (GROUPS, PIECES, 4, depth, rows // PIECES, block)
        dma = pltpu.SemaphoreType.DMA
        return pl.pallas_call(
            functools.partial(solve_kernel, depth, n_gx, n_gy, n_z),
            out_shape=[pltpu.VMEM((cases, width), F32)] * 2,
            in_specs=[smem, smem, smem, vmem, vmem, hbm, hbm, hbm],
            out_specs=[vmem, vmem],
            scratch_shapes=[
                pltpu.VMEM((slots, block, block), F32),
                pltpu.VMEM((slots, block, block), BF16),
                pltpu.VMEM((slots, block, block), F8),
                pltpu.VMEM((slots, block, block), BF16),
                pltpu.VMEM((slots, block, block), F8),
                pltpu.VMEM((3, GROUPS, blocks, rows, block), F32),
                pltpu.VMEM((GROUPS, blocks, rows, block), F32),
                pltpu.VMEM((GROUPS, extent, 2 * rows, block), BF16),
                pltpu.VMEM((GROUPS, blocks, 2 * rows, block), BF16),
                pltpu.VMEM((slots, rows, block), F32),
                pltpu.VMEM((GROUPS, blocks, rows, block), F32),
                pltpu.VMEM((GROUPS, blocks, rows, block), F32),
                pltpu.VMEM((GROUPS, rows, 128), F32),
                pltpu.VMEM((GROUPS, 1, rows, 128), F32),
                pltpu.VMEM(halo, F32),
                pltpu.VMEM(halo, F32),
                pltpu.VMEM(halo, F32),
                [[pltpu.VMEM(halo[2:], F32)] * PIECES] * GROUPS,
                pltpu.VMEM((2, GROUPS, 3, 1, 128), F32),
                pltpu.VMEM((2, GROUPS, peers, 1, 128), F32),
                pltpu.VMEM((16, 128), jnp.int32),
                pltpu.SMEM((16, 128), jnp.int32),
                pltpu.SMEM((4 * blocks,), jnp.int32),
                pltpu.SMEM((4 * blocks,), jnp.int32),
                dma((CHUNKS,)),
                dma((2, GROUPS, blocks)),
                dma,
                dma((GROUPS, PIECES, 4)),
                dma((GROUPS, PIECES, 4)),
                dma((GROUPS, PIECES, 4)),
                dma((GROUPS, PIECES, 4)),
                dma((2, GROUPS, peers)),
                dma((2, GROUPS, peers)),
            ],
            compiler_params=pltpu.CompilerParams(
                collective_id=0, has_side_effects=True, vmem_limit_bytes=60 * 1024 * 1024
            ),
            name="solve",
        )(tile_row, tile_col, send_list, mass, moduli, guess, loads, tiles)

    both = ("gx", "gy")
    return jax.shard_map(
        on_device,
        mesh=mesh,
        in_specs=(
            P(None, both), P(None, both), P(both), P(both), P(both, None, None), P(both), P(both), P(both, None, None),
        ),
        out_specs=(P(None, both), P(None, both)),
        check_vma=False,
    )
```
